32 devices in a mesh: dp: 4 (over y, core), mp: 8 (over z, x).
Axes of the slice: x: 2, y: 2, z: 4, core: 2. Of those that a mesh axis runs over, the one named last changes fastest.
Arguments:
- emb_grad: float32 [65536, 7168], P('dp', 'mp'), may hold values from -600 to 600
- mtp_grad: float32 [14336, 7168], P('dp', 'mp'), may hold values from -600 to 600
- emb_groups: int32 [64], replicated, may hold values from 0 to 31
- mtp_groups: int32 [32], replicated, may hold values from 0 to 31
- max_rms: float32 [1], replicated, may hold values from 0.5 to 2
Outputs:
- emb_clipped: bfloat16 [65536, 7168], P(('dp', 'mp'))
- mtp_clipped: bfloat16 [14336, 7168], P('dp', 'mp')
- group_rms: float32 [32], replicated
The draws below stay inside these ranges and needn't reach their ends.
All inputs are finite; a program needn't handle non-finite values.
Results may differ from the reference program's by a relative error of at most 0.005.
Values may be sent and summed in bfloat16 or wider, within the bound.
A program may use at most 192 MiB of HBM per device.

```python
import math
import jax
import jax.numpy as jnp
from jax import lax

D = 7168
V = 65536
CAT = 14336
EMB_BLK = 1024
MTP_BLK = 448
GROUPS = 32
EMB_BLOCKS = 64
MTP_BLOCKS = 32


def scaled_gradient(key, height, breadth):
    keys = jax.random.split(key, 3)
    row_pos = jnp.arange(height, dtype=jnp.float32) / height
    col_pos = jnp.arange(breadth, dtype=jnp.float32) / breadth
    lower, upper = (math.log(0.3), math.log(3.0))
    base = jnp.clip(jax.random.normal(keys[0], (height, breadth), jnp.float32), -6.0, 6.0)
    row_scale = 3.0 ** (1.0 - row_pos) * jnp.exp(jax.random.uniform(keys[1], (height,), jnp.float32, lower, upper))
    col_scale = 1.8 ** col_pos * jnp.exp(jax.random.uniform(keys[2], (breadth,), jnp.float32, lower, upper))
    return base * row_scale[:, None] * col_scale[None, :]


def draw_emb_grad(key, part):
    return scaled_gradient(jax.random.fold_in(key, 11), V, D)


def draw_mtp_grad(key, part):
    return scaled_gradient(jax.random.fold_in(key, 23), CAT, D)


def with_ends(result, rng, low, largest):
    dims = result.shape
    index_at = [jax.random.randint(jax.random.fold_in(rng, axis), (), 0, dims[axis]) for axis in range(len(dims))]
    result = result.at[tuple(index_at)].set(low)
    longest = dims.index(max(dims))
    index_at[longest] = (index_at[longest] + 1) % dims[longest]
    return result.at[tuple(index_at)].set(largest)


def setup_inputs(seed: int = 0) -> dict:
    key_of = jax.random.split(jax.random.key(seed), 6)
    emb_grad = draw_emb_grad(jax.random.fold_in(key_of[5], 71), 0)
    mtp_grad = draw_mtp_grad(jax.random.fold_in(key_of[5], 71), 0)
    emb_groups = with_ends(jax.random.randint(key_of[2], (EMB_BLOCKS,), 0, GROUPS), jax.random.fold_in(key_of[2], 1), 0, GROUPS - 1).astype(jnp.int32)
    mtp_groups = with_ends(jax.random.randint(key_of[3], (MTP_BLOCKS,), 0, GROUPS), jax.random.fold_in(key_of[3], 1), 0, GROUPS - 1).astype(jnp.int32)
    max_rms = jnp.clip(jnp.exp(jax.random.uniform(key_of[4], (1,), jnp.float32, math.log(0.5), math.log(2.0))), 0.5, 2.0)
    return dict(emb_grad=emb_grad, mtp_grad=mtp_grad, emb_groups=emb_groups, mtp_groups=mtp_groups, max_rms=max_rms)


def block_squares(gradient, block_rows):
    blocks = gradient.reshape(gradient.shape[0] // block_rows, block_rows, gradient.shape[1])
    return lax.optimization_barrier(jnp.sum(jnp.square(blocks), axis=(1, 2)))

def membership(labels):
    return (labels[:, None] == jnp.arange(GROUPS, dtype=jnp.int32)[None, :]).astype(jnp.float32)

def reference(emb_grad, mtp_grad, emb_groups, mtp_groups, max_rms):
    embed_member = membership(emb_groups)
    head_member = membership(mtp_groups)
    embed_squares = block_squares(emb_grad, EMB_BLK)
    head_squares = block_squares(mtp_grad, MTP_BLK)
    group_square = lax.optimization_barrier(jnp.sum(embed_squares[:, None] * embed_member, axis=0)) + lax.optimization_barrier(jnp.sum(head_squares[:, None] * head_member, axis=0))
    group_size = lax.optimization_barrier(jnp.sum(embed_member, axis=0)) * jnp.float32(EMB_BLK * D) + lax.optimization_barrier(jnp.sum(head_member, axis=0)) * jnp.float32(MTP_BLK * D)
    group_rms = jnp.sqrt(group_square / jnp.maximum(group_size, 1.0))
    global_norm = jnp.sqrt(jnp.sum(group_square))
    ceiling = max_rms[0] * jnp.sqrt(jnp.float32((V + CAT) * D))
    factor = ceiling / (global_norm + 1e-06)
    emb_low = lax.optimization_barrier(emb_grad.astype(jnp.bfloat16))
    emb_clipped = (emb_low.astype(jnp.float32) * factor).astype(jnp.bfloat16)
    mtp_clipped = (mtp_grad * factor).astype(jnp.bfloat16)
    return (emb_clipped, mtp_clipped, group_rms)
```

```python
import functools

import jax
import jax.numpy as jnp
from jax import lax
from jax.experimental import pallas as pl
from jax.experimental.pallas import tpu as pltpu
from jax.sharding import PartitionSpec as P

EMB_BLK = 1024
MTP_BLK = 448
GROUPS = 32
STRIP = 64


def squares_kernel(x_ref, out_ref):
    height, width = x_ref.shape

    def step(i, total):
        x = x_ref[pl.ds(pl.multiple_of(i * STRIP, STRIP), STRIP), :]
        return total + jnp.sum((x * x).reshape(STRIP // 8, 8, width), axis=0)

    out_ref[0] = lax.fori_loop(0, height // STRIP, step, jnp.zeros((8, width), jnp.float32))


def block_squares(gradient, block_rows):
    rows, width = gradient.shape
    count = rows // block_rows
    sums = pl.pallas_call(
        squares_kernel,
        grid=(count,),
        in_specs=[pl.BlockSpec((block_rows, width), lambda i: (i, 0))],
        out_specs=pl.BlockSpec((1, 8, width), lambda i: (i, 0, 0)),
        out_shape=jax.ShapeDtypeStruct((count, 8, width), jnp.float32),
        cost_estimate=pl.CostEstimate(
            flops=2 * rows * width, bytes_accessed=4 * rows * width, transcendentals=0
        ),
    )(gradient)
    return jnp.sum(sums, axis=(1, 2))


def round_kernel(x_ref, out_ref):
    out_ref[...] = x_ref[...].astype(jnp.bfloat16)


def rounded_rows(by_owner, first, last, tile):
    pieces, _, width = by_owner.shape
    count = last - first
    start = first // tile
    size = pieces * count * width
    return pl.pallas_call(
        round_kernel,
        grid=(count // tile,),
        in_specs=[pl.BlockSpec((pieces, tile, width), lambda i: (0, start + i, 0))],
        out_specs=pl.BlockSpec((pieces, tile, width), lambda i: (0, i, 0)),
        out_shape=jax.ShapeDtypeStruct((pieces, count, width), jnp.bfloat16),
        cost_estimate=pl.CostEstimate(flops=size, bytes_accessed=6 * size, transcendentals=0),
    )(by_owner)


def scale_kernel(factor_ref, x_ref, *refs):
    out_ref = refs[-1]
    pieces, _, width = x_ref.shape
    factor = factor_ref[0]
    for j in range(pieces):
        out_ref[:, j * width : (j + 1) * width] = (
            x_ref[j].astype(jnp.float32) * factor
        ).astype(jnp.bfloat16)


def scale_rows(factor, arrived, out, first, rows, tile):
    pieces, count, width = arrived.shape
    start = first // tile
    in_specs = [
        pl.BlockSpec(memory_space=pltpu.SMEM),
        pl.BlockSpec((pieces, tile, width), lambda i: (0, i, 0)),
    ]
    operands = [factor.reshape(1), arrived]
    aliases = {}
    if out is not None:
        in_specs.append(pl.BlockSpec(memory_space=pl.ANY))
        operands.append(out)
        aliases = {2: 0}
    return pl.pallas_call(
        scale_kernel,
        grid=(count // tile,),
        in_specs=in_specs,
        out_specs=pl.BlockSpec((tile, pieces * width), lambda i: (start + i, 0)),
        out_shape=jax.ShapeDtypeStruct((rows, pieces * width), jnp.bfloat16),
        input_output_aliases=aliases,
        cost_estimate=pl.CostEstimate(
            flops=arrived.size, bytes_accessed=4 * arrived.size, transcendentals=0
        ),
    )(*operands)


def membership(labels):
    return (labels[:, None] == jnp.arange(GROUPS, dtype=jnp.int32)[None, :]).astype(jnp.float32)


def on_device(shards, pieces, emb_grad, mtp_grad, emb_groups, mtp_groups, max_rms):
    shard = lax.axis_index("dp")
    width = emb_grad.shape[1]
    model_width = width * pieces
    total_rows = (emb_grad.shape[0] + mtp_grad.shape[0]) * shards
    rows = emb_grad.shape[0] // pieces
    tile = rows // 32
    cuts = [0, rows // 8, rows - rows // 16, rows]

    def rounded(gradient, k):
        by_owner = gradient.reshape(pieces, rows, width)
        return rounded_rows(by_owner, cuts[k], cuts[k + 1], tile)

    def exchange(low):
        return lax.all_to_all(low, "mp", split_axis=0, concat_axis=0, tiled=True)

    low = rounded(emb_grad, 0)
    arrived = [exchange(low)]

    embed_count = emb_grad.shape[0] // EMB_BLK
    head_count = mtp_grad.shape[0] // MTP_BLK
    embed_labels = lax.dynamic_slice_in_dim(emb_groups, shard * embed_count, embed_count)
    head_labels = lax.dynamic_slice_in_dim(mtp_groups, shard * head_count, head_count)
    emb_later, mtp_later, low = lax.optimization_barrier((emb_grad, mtp_grad, low))
    partial_value = jnp.sum(
        block_squares(emb_later, EMB_BLK)[:, None] * membership(embed_labels), axis=0
    )
    partial_value = partial_value + jnp.sum(
        block_squares(mtp_later, MTP_BLK)[:, None] * membership(head_labels), axis=0
    )
    later = [rounded(emb_later, k) for k in range(1, len(cuts) - 1)]
    partial_value, later = lax.optimization_barrier((partial_value, later))
    group_square = lax.psum(partial_value, ("dp", "mp"))
    group_square, later = lax.optimization_barrier((group_square, later))
    arrived += [exchange(low) for low in later]

    group_size = jnp.sum(membership(emb_groups), axis=0) * jnp.float32(
        EMB_BLK * model_width
    ) + jnp.sum(membership(mtp_groups), axis=0) * jnp.float32(MTP_BLK * model_width)
    group_rms = jnp.sqrt(group_square / jnp.maximum(group_size, 1.0))
    global_norm = jnp.sqrt(jnp.sum(group_square))
    ceiling = max_rms[0] * jnp.sqrt(jnp.float32(total_rows * model_width))
    factor = ceiling / (global_norm + 1e-06)
    head_output = (mtp_grad * factor).astype(jnp.bfloat16)
    out = None
    for k, block in enumerate(arrived):
        out = scale_rows(factor, block, out, cuts[k], rows, tile)
    return (out, head_output, group_rms)


def solution(mesh):
    placed = (P("dp", "mp"), P("dp", "mp"), P(), P(), P())
    return jax.shard_map(
        functools.partial(on_device, mesh.shape["dp"], mesh.shape["mp"]),
        mesh=mesh,
        in_specs=placed,
        out_specs=(P(("dp", "mp"), None), P("dp", "mp"), P()),
        check_vma=False,
    )
```
